32 devices in a mesh: groups: 2 (over y), rows: 4 (over z), sub: 4 (over x, core).
Axes of the slice: x: 2, y: 2, z: 4, core: 2. Of those that a mesh axis runs over, the one named last changes fastest.
Arguments:
- matrix: float32 [16384, 1024], P(('groups', 'rows', 'sub')), parts along dimension 0
- sign_bits: int32 [16384], P(('groups', 'rows', 'sub')), parts along dimension 0, may hold values from 0 to 1
- samples: int32 [8192], P('groups'), parts along dimension 0, may hold values from 0 to 8191
Outputs:
- cholesky_factor: float32 [2048, 1024], P('groups'), parts along dimension 0
The draws below stay inside these ranges and needn't reach their ends.
There are 2 independent parts, one for each index of `groups`. The reference program is written for one: setup_inputs(seed, part) draws one part's arguments, and reference() takes and returns one part's arrays. A program takes and returns all parts, laid end to end along the dimension named above; each array names one. Nothing has to cross between parts.
Inputs may be any that keep to these rules, and one draw needn't show every extreme that they name: `samples`: row numbers of the whole matrix, drawn independently; a row may be drawn more than once.
All inputs are finite; a program needn't handle non-finite values.
Results may differ from the reference program's by a relative error of at most 0.00011.
Values sent between devices are 32-bit elements; how exact they have to be, the bound alone decides.
No kernel may reach another device: no remote copies, remote signals or barrier semaphores. Data moves between devices by JAX's collectives and lax.ppermute only.
A program may use at most 64 MiB of HBM per device.

```python
import math
import jax
import jax.numpy as jnp
from jax import lax

N = 1024
S = 4096
M = 8192


def draw_matrix(key, part):
    streams = jax.random.split(jax.random.fold_in(key, 17), 3)
    column_scale = jnp.exp(jax.random.uniform(streams[0], (N,), jnp.float32, 0.0, math.log(3.0)))
    row_scale = jnp.exp(jax.random.uniform(streams[1], (M,), jnp.float32, 0.0, math.log(10.0)))
    raw_values = jax.random.truncated_normal(streams[2], -6.0, 6.0, (M, N), jnp.float32)
    return raw_values * row_scale[:, None] * column_scale[None, :] * 0.25


def place_ends(result, own_key, low, largest):
    longest = result.shape.index(max(result.shape))
    spots = []
    for shift in (0, 1):
        where = [jax.random.randint(jax.random.fold_in(own_key, axis), (), 0, length) for axis, length in enumerate(result.shape)]
        where[longest] = (where[longest] + shift) % result.shape[longest]
        spots.append(tuple(where))
    return result.at[spots[0]].set(low).at[spots[1]].set(largest)


def setup_inputs(seed: int = 0, part: int = 0) -> dict:
    arg_keys = jax.random.split(jax.random.key(seed), 4)
    part_keys = jax.random.split(jax.random.fold_in(arg_keys[3], part), 4)
    matrix = draw_matrix(jax.random.fold_in(jax.random.fold_in(arg_keys[3], part), 71), part)
    sign_bits = place_ends(jax.random.randint(part_keys[1], (M,), 0, 2), jax.random.fold_in(part_keys[1], 1), 0, 1).astype(jnp.int32)
    samples = place_ends(jax.random.randint(part_keys[2], (S,), 0, M), jax.random.fold_in(part_keys[2], 1), 0, M - 1).astype(jnp.int32)
    return {"matrix": matrix, "sign_bits": sign_bits, "samples": samples}


def hadamard_rows(values):
    extent = values.shape[0]
    columns = values.shape[1]
    stride = 1
    for level in range(extent.bit_length() - 1):
        paired = values.reshape(extent // (2 * stride), 2, stride, columns)
        values = jnp.stack((paired[:, 0] + paired[:, 1], paired[:, 0] - paired[:, 1]), axis=1).reshape(extent, columns)
        stride = stride * 2
    return values

def reference(matrix, sign_bits, samples):
    sign_values = (2 * sign_bits - 1).astype(jnp.float32)
    signed = matrix * sign_values[:, None]
    mixed_rows = hadamard_rows(signed) / jnp.sqrt(jnp.float32(matrix.shape[0]))
    picked = jnp.take(mixed_rows, samples.astype(jnp.int32), axis=0)
    gram_matrix = jnp.dot(picked.T.astype(jnp.float32), picked.astype(jnp.float32), precision=lax.Precision.HIGHEST, preferred_element_type=jnp.float32) / jnp.float32(samples.shape[0])
    return jnp.linalg.cholesky(gram_matrix)
```

```python
import jax
import jax.numpy as jnp
from jax import lax
from jax.experimental import pallas as pl
from jax.experimental.pallas import tpu as pltpu
from jax.sharding import PartitionSpec as P

HIGHEST = lax.Precision.HIGHEST
BLOCK = 128
GROUP = 8


def hadamard_table(extent):
    line_ids = jnp.arange(extent, dtype=jnp.int32)
    correlation = jnp.bitwise_and(line_ids[:, None], line_ids[None, :])
    parity = jnp.zeros((extent, extent), jnp.int32)
    for bit_pos in range(extent.bit_length() - 1):
        parity = parity + jnp.bitwise_and(jnp.right_shift(correlation, bit_pos), 1)
    return (1 - 2 * (parity % 2)).astype(jnp.float32)


def local_transform(values):
    rows_here, columns = values.shape
    inner_size = min(rows_here, 128)
    outer_size = rows_here // inner_size
    blocks = values.reshape(outer_size, inner_size, columns)
    blocks = jnp.einsum("ab,qbn->qan", hadamard_table(inner_size), blocks, precision=HIGHEST)
    blocks = jnp.einsum("pq,qan->pan", hadamard_table(outer_size), blocks, precision=HIGHEST)
    return blocks.reshape(rows_here, columns)


def mix_sources(received):
    return jnp.einsum("ab,bjn->ajn", hadamard_table(received.shape[0]), received, precision=HIGHEST)


def factor_block(block):
    sub_ids = lax.broadcasted_iota(jnp.int32, (GROUP, BLOCK), 0)
    lane_ids = lax.broadcasted_iota(jnp.int32, (GROUP, BLOCK), 1)
    count = BLOCK // GROUP
    rows = [block[GROUP * t : GROUP * (t + 1), :] for t in range(count)]
    extra = [jnp.where(lane_ids == sub_ids + GROUP * t, 1.0, 0.0).astype(jnp.float32) for t in range(count)]
    upper, inverse = [], []

    def spread(value, index):
        return jnp.broadcast_to(value[index : index + 1, :], (GROUP, BLOCK))

    for g in range(count):
        own, aug = rows[g], extra[g]
        cols = [jnp.broadcast_to(own[:, GROUP * g + j : GROUP * g + j + 1], (GROUP, BLOCK)) for j in range(GROUP)]
        own_out, aug_out = own, aug
        for j in range(GROUP):
            factor = cols[j]
            pivot = spread(factor, j)
            root = lax.rsqrt(pivot)
            here = sub_ids == j
            own_row, aug_row = spread(own, j) * root, spread(aug, j) * root
            own_out = jnp.where(here, own_row, own_out)
            aug_out = jnp.where(here, aug_row, aug_out)
            multiplier = jnp.where(here, -root, factor * root)
            own = jnp.where(here, 0.0, own) - multiplier * own_row
            aug = jnp.where(here, 0.0, aug) - multiplier * aug_row
            for m in range(j + 1, GROUP):
                line = spread(cols[m], j) * root
                cols[m] = jnp.where(here, 0.0, cols[m]) - multiplier * line
        upper.append(jnp.where(lane_ids >= sub_ids + GROUP * g, own_out, 0.0))
        inverse.append(aug_out)
        own_lines = [spread(own, j) for j in range(GROUP)]
        aug_lines = [spread(aug, j) for j in range(GROUP)]
        for t in range(g + 1, count):
            source = rows[t]
            own_sum = aug_sum = None
            for j in range(GROUP):
                column = jnp.broadcast_to(source[:, GROUP * g + j : GROUP * g + j + 1], (GROUP, BLOCK))
                own_term, aug_term = column * own_lines[j], column * aug_lines[j]
                own_sum = own_term if own_sum is None else own_sum + own_term
                aug_sum = aug_term if aug_sum is None else aug_sum + aug_term
            rows[t] = source - own_sum
            extra[t] = extra[t] - aug_sum
    return jnp.concatenate(upper, axis=0), jnp.concatenate(inverse, axis=0)


def transposed_dot(left, right):
    return lax.dot_general(
        left, right, (((0,), (0,)), ((), ())), precision=HIGHEST, preferred_element_type=jnp.float32
    )


def panel_kernel(offset, columns, last, *refs):
    gram_ref, *earlier = refs[: -2 if last else -1]
    out_ref = refs[-2] if last else refs[-1]
    own_ref = refs[-1]
    height, width = gram_ref.shape
    current = gram_ref[...]
    for ref in earlier:
        skip = ref.shape[1] - width
        current = current - transposed_dot(ref[:, skip : skip + height], ref[:, skip:])
    own_ref[...] = current
    steps = height // BLOCK

    def step(k):
        base = BLOCK * k
        upper, inverse = factor_block(own_ref[base : base + BLOCK, base : base + BLOCK])
        own_ref[base : base + BLOCK, base : base + BLOCK] = upper
        right = base + BLOCK
        if right < width:
            solved = jnp.dot(
                inverse, own_ref[base : base + BLOCK, right:], precision=HIGHEST, preferred_element_type=jnp.float32
            )
            own_ref[base : base + BLOCK, right:] = solved
            if right < height:
                own_ref[right:, right:] = own_ref[right:, right:] - transposed_dot(
                    solved[:, : height - right], solved
                )
        if base:
            own_ref[base : base + BLOCK, :base] = jnp.zeros((BLOCK, base), jnp.float32)

    for k in range(steps):
        step(k)
    if last:
        out_ref[...] = jnp.zeros((columns, columns), jnp.float32)
        for ref in [*earlier, own_ref]:
            tall, wide = ref.shape
            start = columns - wide
            out_ref[start:, start : start + tall] = ref[...].T


def factor_panel(gram_rows, earlier, columns):
    height, width = gram_rows.shape
    last = height == width
    args = 1 + len(earlier)
    scratch = [pltpu.VMEM((height, width), jnp.float32)] if last else []
    shape = (columns, columns) if last else (height, width)

    def kernel(*refs):
        panel_kernel(columns - width, columns, last, *refs)

    return pl.pallas_call(
        kernel,
        out_shape=jax.ShapeDtypeStruct(shape, jnp.float32),
        in_specs=[pl.BlockSpec(memory_space=pltpu.VMEM)] * args,
        out_specs=pl.BlockSpec(memory_space=pltpu.VMEM),
        scratch_shapes=scratch,
        compiler_params=pltpu.CompilerParams(vmem_limit_bytes=48 * 1024 * 1024),
    )(gram_rows, *earlier)


def body(matrix, sign_bits, samples):
    rows_here, columns = matrix.shape
    devices = lax.axis_size(("rows", "sub"))
    position = lax.axis_index(("rows", "sub"))
    per_block = rows_here // devices
    sign_values = (2 * sign_bits - 1).astype(jnp.float32)
    current = local_transform(matrix * sign_values[:, None])
    block_ids = (
        (jnp.arange(devices, dtype=jnp.int32) * rows_here)[:, None]
        + position * per_block
        + jnp.arange(per_block, dtype=jnp.int32)[None, :]
    )
    blocks = current.reshape(devices, per_block, columns)
    mixed_rows = mix_sources(
        lax.all_to_all(blocks, ("rows", "sub"), split_axis=0, concat_axis=0, tiled=True)
    )
    owned_rows = mixed_rows.reshape(rows_here, columns)
    row_ids = block_ids.reshape(rows_here)
    matches = (row_ids[:, None] == samples[None, :]).astype(jnp.float32)
    counts = jnp.sum(matches, axis=1) / jnp.float32(rows_here * devices * samples.shape[0])
    weighted = owned_rows * counts[:, None]
    height = columns // 4
    summed = []
    for start in range(0, columns, height):
        own = jnp.einsum(
            "rn,rm->nm", weighted[:, start : start + height], owned_rows[:, start:], precision=HIGHEST
        )
        if summed:
            own, summed[-1] = lax.optimization_barrier((own, summed[-1]))
        summed.append(lax.psum(own, ("rows", "sub")))
    panels = []
    for gram_rows in summed:
        panels.append(factor_panel(gram_rows, panels, columns))
    return panels[-1]


def solution(mesh):
    placed = (P(("groups", "rows", "sub"), None), P(("groups", "rows", "sub")), P("groups"))
    return jax.shard_map(
        body, mesh=mesh, in_specs=placed, out_specs=P("groups", None), check_vma=False
    )
```

```python
import jax
import jax.numpy as jnp
from jax import lax
from jax.experimental import pallas as pl
from jax.experimental.pallas import tpu as pltpu
from jax.sharding import PartitionSpec as P

HIGHEST = lax.Precision.HIGHEST
BLOCK = 128
GROUP = 8


def hadamard_table(extent):
    line_ids = jnp.arange(extent, dtype=jnp.int32)
    correlation = jnp.bitwise_and(line_ids[:, None], line_ids[None, :])
    parity = jnp.zeros((extent, extent), jnp.int32)
    for bit_pos in range(extent.bit_length() - 1):
        parity = parity + jnp.bitwise_and(jnp.right_shift(correlation, bit_pos), 1)
    return (1 - 2 * (parity % 2)).astype(jnp.float32)


def local_transform(values):
    rows_here, columns = values.shape
    inner_size = min(rows_here, 128)
    outer_size = rows_here // inner_size
    blocks = values.reshape(outer_size, inner_size, columns)
    blocks = jnp.einsum("ab,qbn->qan", hadamard_table(inner_size), blocks, precision=HIGHEST)
    blocks = jnp.einsum("pq,qan->pan", hadamard_table(outer_size), blocks, precision=HIGHEST)
    return blocks.reshape(rows_here, columns)


def mix_sources(received):
    return jnp.einsum("ab,bjn->ajn", hadamard_table(received.shape[0]), received, precision=HIGHEST)


def factor_block(block):
    sub_ids = lax.broadcasted_iota(jnp.int32, (GROUP, BLOCK), 0)
    lane_ids = lax.broadcasted_iota(jnp.int32, (GROUP, BLOCK), 1)
    count = BLOCK // GROUP
    rows = [block[GROUP * t : GROUP * (t + 1), :] for t in range(count)]
    extra = [jnp.where(lane_ids == sub_ids + GROUP * t, 1.0, 0.0).astype(jnp.float32) for t in range(count)]
    upper, inverse = [], []

    def spread(value, index):
        return jnp.broadcast_to(value[index : index + 1, :], (GROUP, BLOCK))

    for g in range(count):
        own, aug = rows[g], extra[g]
        cols = [jnp.broadcast_to(own[:, GROUP * g + j : GROUP * g + j + 1], (GROUP, BLOCK)) for j in range(GROUP)]
        own_out, aug_out = own, aug
        for j in range(GROUP):
            factor = cols[j]
            pivot = spread(factor, j)
            root = lax.rsqrt(pivot)
            here = sub_ids == j
            own_row, aug_row = spread(own, j) * root, spread(aug, j) * root
            own_out = jnp.where(here, own_row, own_out)
            aug_out = jnp.where(here, aug_row, aug_out)
            multiplier = jnp.where(here, -root, factor * root)
            own = jnp.where(here, 0.0, own) - multiplier * own_row
            aug = jnp.where(here, 0.0, aug) - multiplier * aug_row
            for m in range(j + 1, GROUP):
                line = spread(cols[m], j) * root
                cols[m] = jnp.where(here, 0.0, cols[m]) - multiplier * line
        upper.append(jnp.where(lane_ids >= sub_ids + GROUP * g, own_out, 0.0))
        inverse.append(aug_out)
        own_lines = [spread(own, j) for j in range(GROUP)]
        aug_lines = [spread(aug, j) for j in range(GROUP)]
        for t in range(g + 1, count):
            source = rows[t]
            own_sum = aug_sum = None
            for j in range(GROUP):
                column = jnp.broadcast_to(source[:, GROUP * g + j : GROUP * g + j + 1], (GROUP, BLOCK))
                own_term, aug_term = column * own_lines[j], column * aug_lines[j]
                own_sum = own_term if own_sum is None else own_sum + own_term
                aug_sum = aug_term if aug_sum is None else aug_sum + aug_term
            rows[t] = source - own_sum
            extra[t] = extra[t] - aug_sum
    return jnp.concatenate(upper, axis=0), jnp.concatenate(inverse, axis=0)


def transposed_dot(left, right):
    return lax.dot_general(
        left, right, (((0,), (0,)), ((), ())), precision=HIGHEST, preferred_element_type=jnp.float32
    )


def panel_kernel(offset, columns, last, *refs):
    gram_ref, *earlier = refs[: -2 if last else -1]
    out_ref = refs[-2] if last else refs[-1]
    own_ref = refs[-1]
    height, width = gram_ref.shape
    current = gram_ref[...]
    for ref in earlier:
        skip = ref.shape[1] - width
        current = current - transposed_dot(ref[:, skip : skip + height], ref[:, skip:])
    own_ref[...] = current
    steps = height // BLOCK

    def step(k):
        base = BLOCK * k
        upper, inverse = factor_block(own_ref[base : base + BLOCK, base : base + BLOCK])
        own_ref[base : base + BLOCK, base : base + BLOCK] = upper
        right = base + BLOCK
        if right < width:
            solved = jnp.dot(
                inverse, own_ref[base : base + BLOCK, right:], precision=HIGHEST, preferred_element_type=jnp.float32
            )
            own_ref[base : base + BLOCK, right:] = solved
            if right < height:
                own_ref[right:, right:] = own_ref[right:, right:] - transposed_dot(
                    solved[:, : height - right], solved
                )
        if base:
            own_ref[base : base + BLOCK, :base] = jnp.zeros((BLOCK, base), jnp.float32)

    for k in range(steps):
        step(k)
    if last:
        out_ref[...] = jnp.zeros((columns, columns), jnp.float32)
        for ref in [*earlier, own_ref]:
            tall, wide = ref.shape
            start = columns - wide
            out_ref[start:, start : start + tall] = ref[...].T


def factor_panel(gram_rows, earlier, columns):
    height, width = gram_rows.shape
    last = height == width
    args = 1 + len(earlier)
    scratch = [pltpu.VMEM((height, width), jnp.float32)] if last else []
    shape = (columns, columns) if last else (height, width)

    def kernel(*refs):
        panel_kernel(columns - width, columns, last, *refs)

    return pl.pallas_call(
        kernel,
        out_shape=jax.ShapeDtypeStruct(shape, jnp.float32),
        in_specs=[pl.BlockSpec(memory_space=pltpu.VMEM)] * args,
        out_specs=pl.BlockSpec(memory_space=pltpu.VMEM),
        scratch_shapes=scratch,
        compiler_params=pltpu.CompilerParams(vmem_limit_bytes=48 * 1024 * 1024),
    )(gram_rows, *earlier)


def body(matrix, sign_bits, samples):
    rows_here, columns = matrix.shape
    devices = lax.axis_size(("rows", "sub"))
    position = lax.axis_index(("rows", "sub"))
    per_block = rows_here // devices
    sign_values = (2 * sign_bits - 1).astype(jnp.float32)
    current = local_transform(matrix * sign_values[:, None])
    block_ids = (
        (jnp.arange(devices, dtype=jnp.int32) * rows_here)[:, None]
        + position * per_block
        + jnp.arange(per_block, dtype=jnp.int32)[None, :]
    )
    blocks = current.reshape(devices, per_block, columns)
    mixed_rows = mix_sources(
        lax.all_to_all(blocks, ("rows", "sub"), split_axis=0, concat_axis=0, tiled=True)
    )
    owned_rows = mixed_rows.reshape(rows_here, columns)
    row_ids = block_ids.reshape(rows_here)
    matches = (row_ids[:, None] == samples[None, :]).astype(jnp.float32)
    counts = jnp.sum(matches, axis=1) / jnp.float32(rows_here * devices * samples.shape[0])
    weighted = owned_rows * counts[:, None]
    height = columns // 4
    shares = [
        jnp.einsum("rn,rm->nm", weighted[:, start : start + height], owned_rows[:, start:], precision=HIGHEST)
        for start in range(0, columns, height)
    ]
    half = height // 2
    packed = jnp.concatenate(
        [
            shares[0],
            jnp.concatenate([shares[1], shares[3]], axis=1),
            jnp.concatenate([shares[2][:half], shares[2][half:]], axis=1),
        ],
        axis=0,
    )
    packed = lax.psum(packed, ("rows", "sub"))
    middle = packed[height : 2 * height]
    tail = packed[2 * height :]
    summed = [
        packed[:height],
        middle[:, : 3 * height],
        jnp.concatenate([tail[:, : 2 * height], tail[:, 2 * height :]], axis=0),
        middle[:, 3 * height :],
    ]
    panels = []
    for gram_rows in summed:
        panels.append(factor_panel(gram_rows, panels, columns))
    return panels[-1]


def solution(mesh):
    placed = (P(("groups", "rows", "sub"), None), P(("groups", "rows", "sub")), P("groups"))
    return jax.shard_map(
        body, mesh=mesh, in_specs=placed, out_specs=P("groups", None), check_vma=False
    )
```
